16 devices in a mesh: dp: 4 (over z, y), ep: 4 (over x, core).
Axes of the slice: x: 2, y: 2, z: 2, core: 2. Of those that a mesh axis runs over, the one named last changes fastest.
Arguments:
- x_tok: bfloat16 [1024, 1536], P(('dp', 'ep')), parts along dimension 0
- topk_idx: int32 [1024, 6], P(('dp', 'ep')), parts along dimension 0
- topk_w: float32 [1024, 6], P(('dp', 'ep')), parts along dimension 0
- w_in: bfloat16 [64, 1536, 512], P('ep')
- w_out: bfloat16 [64, 512, 1536], P('ep')
- shared_in: bfloat16 [1536, 1024], replicated
- shared_out: bfloat16 [1024, 1536], replicated
Outputs:
- output: bfloat16 [1024, 1536], P(('dp', 'ep')), parts along dimension 0
There are 4 independent parts. The reference program is written for one: setup_inputs(seed, part) draws one part's arguments, and reference() takes and returns one part's arrays. A program takes and returns all parts, laid end to end along the dimension named above; an argument that names none is the same for every part.
All inputs are finite; a program needn't handle non-finite values.
Results may differ from the reference program's by a relative error of at most 0.001.
Values are sent between devices in bfloat16 or wider.
A program may use at most 1 GiB of HBM per device.

```python
import jax
import jax.numpy as jnp
from jax import lax

GROUP_SIZE = 4
TOK_DEV = 64
D_MODEL = 1536
FF_DIM = 512
FS_DIM = 1024
EXPERTS = 64
TOP_K = 6
NUM_HOT = 2
SLOT_CAP = 18

TOKENS = GROUP_SIZE * TOK_DEV
EXPERT_ROWS = SLOT_CAP * GROUP_SIZE


def draw_routing(route_key):
    key_hot, key_extra, key_tok, key_rot = jax.random.split(route_key, 4)
    cold_count = EXPERTS - NUM_HOT
    rest_pairs = TOK_DEV * TOP_K - NUM_HOT * SLOT_CAP
    base_load = rest_pairs // cold_count
    extra_pairs = rest_pairs - base_load * cold_count
    expert_order = jax.random.permutation(key_hot, EXPERTS)
    cold_rank = jax.vmap(lambda dev_key: jax.random.permutation(dev_key, cold_count))(jax.random.split(key_extra, GROUP_SIZE))
    cold_load = base_load + (cold_rank < extra_pairs).astype(jnp.int32)
    hot_load = jnp.full((GROUP_SIZE, NUM_HOT), SLOT_CAP, jnp.int32)
    ordered_load = jnp.concatenate([hot_load, cold_load], axis=1)
    expert_load = jnp.zeros((GROUP_SIZE, EXPERTS), jnp.int32).at[:, expert_order].set(ordered_load)
    load_ends = jnp.cumsum(expert_load, axis=1)
    pair_ids = jnp.arange(TOK_DEV * TOP_K, dtype=jnp.int32)
    pair_expert = jax.vmap(lambda ends_row: jnp.searchsorted(ends_row, pair_ids, side='right'))(load_ends)
    slot_table = pair_expert.reshape(GROUP_SIZE, TOP_K, TOK_DEV).transpose(0, 2, 1)
    tok_perm = jax.vmap(lambda dev_key: jax.random.permutation(dev_key, TOK_DEV))(jax.random.split(key_tok, GROUP_SIZE))
    tok_index = jnp.broadcast_to(tok_perm[:, :, None], (GROUP_SIZE, TOK_DEV, TOP_K))
    slot_table = jnp.take_along_axis(slot_table, tok_index, axis=1)
    slot_shift = jax.random.randint(key_rot, (GROUP_SIZE, TOK_DEV, 1), 0, TOP_K)
    slot_cols = (jnp.arange(TOP_K)[None, None, :] + slot_shift) % TOP_K
    slot_table = jnp.take_along_axis(slot_table, slot_cols, axis=2)
    return slot_table.reshape(TOKENS, TOP_K).astype(jnp.int32)


def draw_stack(stack_key, fan_in, fan_out):
    def one_expert(expert_key):
        return (jax.random.normal(expert_key, (fan_in, fan_out), jnp.float32) * fan_in ** -0.5).astype(jnp.bfloat16)
    return lax.map(one_expert, jax.random.split(stack_key, EXPERTS))


def setup_inputs(seed: int = 0, part: int = 0) -> dict:
    root_key = jax.random.key(seed)
    key_x, key_route, key_gate, key_in, key_out, key_sin, key_sout = jax.random.split(root_key, 7)
    x_tok = jax.random.normal(jax.random.fold_in(key_x, part), (TOKENS, D_MODEL), jnp.float32).astype(jnp.bfloat16)
    topk_idx = draw_routing(jax.random.fold_in(key_route, part))
    gate_raw = jax.random.uniform(jax.random.fold_in(key_gate, part), (TOKENS, TOP_K), jnp.float32, 0.2, 1.0)
    topk_w = gate_raw * (1.5 / TOP_K ** 0.5)
    w_in = draw_stack(key_in, D_MODEL, FF_DIM)
    w_out = draw_stack(key_out, FF_DIM, D_MODEL)
    shared_in = (jax.random.normal(key_sin, (D_MODEL, FS_DIM), jnp.float32) * D_MODEL ** -0.5).astype(jnp.bfloat16)
    shared_out = (jax.random.normal(key_sout, (FS_DIM, D_MODEL), jnp.float32) * FS_DIM ** -0.5).astype(jnp.bfloat16)
    return {'x_tok': x_tok, 'topk_idx': topk_idx, 'topk_w': topk_w, 'w_in': w_in, 'w_out': w_out, 'shared_in': shared_in, 'shared_out': shared_out}


def reference(x_tok, topk_idx, topk_w, w_in, w_out, shared_in, shared_out):
    pair_total = TOKENS * TOP_K
    flat_ids = topk_idx.reshape(pair_total)
    pair_order = jnp.argsort(flat_ids, stable=True)
    counts = jnp.zeros((EXPERTS,), jnp.int32).at[flat_ids].add(1)
    starts = jnp.cumsum(counts) - counts
    pair_gates = topk_w.astype(jnp.bfloat16).astype(jnp.float32).reshape(pair_total)
    slot_ids = jnp.arange(EXPERT_ROWS)

    def expert_step(routed_acc, step_in):
        e_index, w_first, w_second = step_in
        slot_valid = slot_ids < counts[e_index]
        pair_pos = pair_order[jnp.minimum(starts[e_index] + slot_ids, pair_total - 1)]
        tok_pos = pair_pos // TOP_K
        gathered = x_tok[tok_pos]
        hidden = jax.nn.gelu(jnp.dot(gathered, w_first, preferred_element_type=jnp.float32), approximate=True).astype(jnp.bfloat16)
        expert_out = jnp.dot(hidden, w_second, preferred_element_type=jnp.float32).astype(jnp.bfloat16)
        pair_scale = jnp.where(slot_valid, pair_gates[pair_pos], 0.0)
        contrib = expert_out.astype(jnp.float32) * pair_scale[:, None]
        return routed_acc.at[tok_pos].add(contrib), None

    routed_init = jnp.zeros((TOKENS, D_MODEL), jnp.float32)
    routed, _ = lax.scan(expert_step, routed_init, (jnp.arange(EXPERTS), w_in, w_out))
    shared_hidden = jax.nn.gelu(jnp.dot(x_tok, shared_in, preferred_element_type=jnp.float32), approximate=True).astype(jnp.bfloat16)
    shared_val = jnp.dot(shared_hidden, shared_out, preferred_element_type=jnp.float32)
    return (routed + shared_val).astype(jnp.bfloat16)
```

```python
import functools
import math

import jax
import jax.numpy as jnp
from jax import lax
from jax.experimental import pallas as pl
from jax.experimental.pallas import tpu as pltpu
from jax.sharding import PartitionSpec as P

MESH = pl.DeviceIdType.MESH
LOAD_MULT = 3
COLS = 256
GELU_A = math.sqrt(2.0 / math.pi)
GELU_B = GELU_A * 0.044715


def gelu(z):
    return 0.5 * z * (1.0 + jnp.tanh(z * (GELU_A + GELU_B * (z * z))))


def dot(a, b):
    return jnp.dot(a, b, preferred_element_type=jnp.float32)


def layer_kernel(
    dims,
    x_hbm, idx_hbm, gate_hbm, win_hbm, wout_hbm, sin_hbm, sout_hbm,
    y_hbm,
    x_all, win, wout, idx_all, gate_all, disp, comb, rows_in, acc, hidden, rows_out,
    part, sib_part, sib_fwd, link_out, link_in, y_buf, shared_h, shared_u,
    small_sem, x_sem, win_sem, wout_sem, shared_sem, y_sem,
    meta_send, meta_recv, xl_send, xl_recv, xs_send, xs_recv, xf_send, xf_recv,
    ps_send, ps_recv, pf_send, pf_recv, pl_send, pl_recv,
):
    tok, top_k, local_e, slot, tokens = dims
    d_model, ff = win_hbm.shape[1], win_hbm.shape[2]
    chunks = d_model // COLS
    me = lax.axis_index('ep')
    chip, core = lax.div(me, 2), lax.rem(me, 2)
    sib = chip * 2 + (1 - core)
    mir = (1 - chip) * 2 + core
    diag = (1 - chip) * 2 + (1 - core)
    peers = (sib, mir, diag)

    def rows_of(dev):
        return pl.ds(pl.multiple_of(dev * tok, tok), tok)

    def remote(src, dst, send, recv, dev):
        return pltpu.make_async_remote_copy(
            src_ref=src, dst_ref=dst, send_sem=send, recv_sem=recv,
            device_id={'ep': dev}, device_id_type=MESH)

    idx_cp = pltpu.make_async_copy(idx_hbm, idx_all.at[me], small_sem.at[0])
    gate_cp = pltpu.make_async_copy(gate_hbm, gate_all.at[me], small_sem.at[1])
    idx_cp.start()
    gate_cp.start()
    x_cps = [pltpu.make_async_copy(x_hbm.at[:, pl.ds(k * COLS, COLS)], x_all.at[k, rows_of(me)], x_sem.at[k]) for k in range(chunks)]
    for cp in x_cps:
        cp.start()
    win_cps = [pltpu.make_async_copy(win_hbm.at[:, pl.ds(k * COLS, COLS), :], win.at[k], win_sem.at[k]) for k in range(chunks)]
    for cp in win_cps:
        cp.start()
    wout_cps = [pltpu.make_async_copy(wout_hbm.at[:, :, pl.ds(n * COLS, COLS)], wout.at[n], wout_sem.at[n]) for n in range(chunks)]
    for cp in wout_cps:
        cp.start()

    barrier = pltpu.get_barrier_semaphore()
    for peer in peers:
        pl.semaphore_signal(barrier, inc=1, device_id={'ep': peer}, device_id_type=MESH)

    idx_cp.wait()
    gate_cp.wait()
    pl.semaphore_wait(barrier, 3)
    meta_cps = []
    for r, peer in enumerate(peers):
        meta_cps.append(remote(idx_all.at[me], idx_all.at[me], meta_send.at[r], meta_recv.at[r], peer))
        meta_cps.append(remote(gate_all.at[me], gate_all.at[me], meta_send.at[3 + r], meta_recv.at[3 + r], peer))
    for cp in meta_cps:
        cp.start()
    xl_cps, xs_cps, xf_cps = [], [], []
    for k in range(chunks):
        mine, theirs = x_all.at[k, rows_of(me)], x_all.at[k, rows_of(mir)]
        xl_cps.append(remote(mine, mine, xl_send.at[k], xl_recv.at[k], mir))
        xs_cps.append(remote(mine, mine, xs_send.at[k], xs_recv.at[k], sib))
        xf_cps.append(remote(theirs, theirs, xf_send.at[k], xf_recv.at[k], sib))
    for k in range(chunks):
        x_cps[k].wait()
        xl_cps[k].start()
        xs_cps[k].start()

    for cp in meta_cps:
        cp.wait_recv()
    group = tokens // tok
    idx_t = jnp.concatenate([idx_all[s] for s in range(group)], axis=1)
    gate_t = jnp.concatenate([gate_all[s] for s in range(group)], axis=1).astype(jnp.bfloat16).astype(jnp.float32)
    expert_id = lax.broadcasted_iota(jnp.int32, (local_e, tokens), 0) + me * local_e
    picked = jnp.zeros((local_e, tokens), jnp.float32)
    gates = jnp.zeros((local_e, tokens), jnp.float32)
    for j in range(top_k):
        hit = idx_t[j:j + 1, :] == expert_id
        picked = picked + jnp.where(hit, 1.0, 0.0)
        gates = gates + jnp.where(hit, gate_t[j:j + 1, :], 0.0)
    before = (lax.broadcasted_iota(jnp.int32, (tokens, tokens), 0) < lax.broadcasted_iota(jnp.int32, (tokens, tokens), 1))
    rank = dot(picked.astype(jnp.bfloat16), jnp.where(before, 1.0, 0.0).astype(jnp.bfloat16))
    rank = jnp.where(picked > 0.5, rank, -1.0)
    slot_id = lax.broadcasted_iota(jnp.int32, (slot, tokens), 0).astype(jnp.float32)
    for e in range(local_e):
        here = slot_id == rank[e:e + 1, :]
        disp[pl.ds(e * slot, slot), :] = jnp.where(here, 1.0, 0.0).astype(jnp.bfloat16)
        rows_out[pl.ds(e * slot, slot), :] = jnp.where(here, gates[e:e + 1, :], 0.0).astype(jnp.bfloat16)
    for i in range(local_e * slot // 256):
        comb[:, pl.ds(i * 256, 256)] = rows_out[pl.ds(i * 256, 256), :].T

    xl_cps[0].wait_recv()
    xf_cps[0].start()
    for k in range(chunks):
        if k + 1 < chunks:
            xl_cps[k + 1].wait_recv()
            xf_cps[k + 1].start()
        xs_cps[k].wait_recv()
        xf_cps[k].wait_recv()
        rows_in[...] = dot(disp[...], x_all[k]).astype(jnp.bfloat16)
        win_cps[k].wait()
        for e in range(local_e):
            r = pl.ds(e * slot, slot)
            term = dot(rows_in[r, :], win[k, e])
            if k == 0:
                acc[r, :] = term
            elif k + 1 < chunks:
                acc[r, :] = acc[r, :] + term
            else:
                hidden[r, :] = gelu(acc[r, :] + term).astype(jnp.bfloat16)

    shared_cps = []
    for k in range(chunks):
        for j in range(2):
            shared_cps.append(pltpu.make_async_copy(
                sin_hbm.at[pl.ds(k * COLS, COLS), pl.ds(j * ff, ff)], win.at[k, j], shared_sem.at[k * 2 + j]))
    for i in range(4):
        for j in range(3):
            shared_cps.append(pltpu.make_async_copy(
                sout_hbm.at[pl.ds(i * COLS, COLS), pl.ds(j * ff, ff)], win.at[i, 2 + j], shared_sem.at[12 + i * 3 + j]))
    for cp in shared_cps:
        cp.start()

    ps_cps = [remote(part.at[n, rows_of(sib)], sib_part.at[n], ps_send.at[n], ps_recv.at[n], sib) for n in range(chunks)]
    pf_cps = [remote(part.at[n, rows_of(diag)], sib_fwd.at[n], pf_send.at[n], pf_recv.at[n], sib) for n in range(chunks)]
    pl_cps = [remote(link_out.at[n], link_in.at[n], pl_send.at[n], pl_recv.at[n], mir) for n in range(chunks)]

    def send_back(n):
        pf_cps[n].wait_recv()
        link_out[n] = part[n, rows_of(mir), :] + sib_fwd[n]
        pl_cps[n].start()

    for n in range(chunks):
        wout_cps[n].wait()
        for e in range(local_e):
            r = pl.ds(e * slot, slot)
            rows_out[r, :] = dot(hidden[r, :], wout[n, e]).astype(jnp.bfloat16)
        part[n] = dot(comb[...], rows_out[...])
        pf_cps[n].start()
        ps_cps[n].start()
        if n:
            send_back(n - 1)
    send_back(chunks - 1)

    for cp in shared_cps:
        cp.wait()
    for j in range(2):
        s = dot(x_all[0, rows_of(me), :], win[0, j])
        for k in range(1, chunks):
            s = s + dot(x_all[k, rows_of(me), :], win[k, j])
        shared_h[:, pl.ds(j * ff, ff)] = gelu(s).astype(jnp.bfloat16)
    for j in range(3):
        u = dot(shared_h[:, 0:COLS], win[0, 2 + j])
        for i in range(1, 4):
            u = u + dot(shared_h[:, pl.ds(i * COLS, COLS)], win[i, 2 + j])
        shared_u[:, pl.ds(j * ff, ff)] = u

    y_cps = [pltpu.make_async_copy(y_buf.at[n], y_hbm.at[:, pl.ds(n * COLS, COLS)], y_sem.at[n]) for n in range(chunks)]
    for n in range(chunks):
        ps_cps[n].wait_recv()
        mine = shared_u[:, pl.ds(n * COLS, COLS)] + part[n, rows_of(me), :] + sib_part[n]
        pl_cps[n].wait_recv()
        y_buf[n] = (mine + link_in[n]).astype(jnp.bfloat16)
        y_cps[n].start()
    for cp in meta_cps + xl_cps + xs_cps + xf_cps + ps_cps + pf_cps + pl_cps:
        cp.wait_send()
    for cp in y_cps:
        cp.wait()


def solution(mesh):
    group = mesh.shape['ep']

    def local_layer(x_loc, idx_loc, gate_loc, w_in, w_out, shared_in, shared_out):
        tok, top_k = idx_loc.shape
        local_e, d_model, ff = w_in.shape
        fs = shared_in.shape[1]
        tokens = tok * group
        cap = min(tok, LOAD_MULT * tok * top_k // (local_e * group))
        slot = -(-cap * group // 16) * 16
        total = local_e * slot
        chunks = d_model // COLS
        bf16, f32 = jnp.bfloat16, jnp.float32
        dma = pltpu.SemaphoreType.DMA
        scratch = [
            pltpu.VMEM((chunks, tokens, COLS), bf16),
            pltpu.VMEM((chunks, local_e, COLS, ff), bf16),
            pltpu.VMEM((chunks, local_e, ff, COLS), bf16),
            pltpu.VMEM((group, top_k, tok), jnp.int32),
            pltpu.VMEM((group, top_k, tok), f32),
            pltpu.VMEM((total, tokens), bf16),
            pltpu.VMEM((tokens, total), bf16),
            pltpu.VMEM((total, COLS), bf16),
            pltpu.VMEM((total, ff), f32),
            pltpu.VMEM((total, ff), bf16),
            pltpu.VMEM((total, COLS), bf16),
            pltpu.VMEM((chunks, tokens, COLS), f32),
            pltpu.VMEM((chunks, tok, COLS), f32),
            pltpu.VMEM((chunks, tok, COLS), f32),
            pltpu.VMEM((chunks, tok, COLS), f32),
            pltpu.VMEM((chunks, tok, COLS), f32),
            pltpu.VMEM((chunks, tok, COLS), bf16),
            pltpu.VMEM((tok, fs), bf16),
            pltpu.VMEM((tok, d_model), f32),
            dma((2,)), dma((chunks,)), dma((chunks,)), dma((chunks,)), dma((24,)), dma((chunks,)),
            dma((6,)), dma((6,)),
        ] + [dma((chunks,))] * 12
        any_spec = pl.BlockSpec(memory_space=pl.ANY)
        return pl.pallas_call(
            functools.partial(layer_kernel, (tok, top_k, local_e, slot, tokens)),
            out_shape=jax.ShapeDtypeStruct((tok, d_model), bf16),
            in_specs=[any_spec] * 7,
            out_specs=any_spec,
            scratch_shapes=scratch,
            compiler_params=pltpu.CompilerParams(
                collective_id=0, has_side_effects=True, vmem_limit_bytes=67043328),
        )(x_loc, idx_loc.T, gate_loc.T, w_in, w_out, shared_in, shared_out)

    tok_spec = P(('dp', 'ep'), None)
    expert_spec = P('ep', None, None)
    whole_spec = P(None, None)
    return jax.shard_map(
        local_layer, mesh=mesh,
        in_specs=(tok_spec, tok_spec, tok_spec, expert_spec, expert_spec, whole_spec, whole_spec),
        out_specs=tok_spec, check_vma=False)
```

```python
import functools
import math

import jax
import jax.numpy as jnp
from jax import lax
from jax.experimental import pallas as pl
from jax.experimental.pallas import tpu as pltpu
from jax.sharding import PartitionSpec as P

MESH = pl.DeviceIdType.MESH
LOAD_MULT = 3
VMEM_LIMIT = 61500000
scope = jax.named_scope
COLS = 256
GELU_A = math.sqrt(2.0 / math.pi)
GELU_B = GELU_A * 0.044715


def gelu(z):
    return 0.5 * z * (1.0 + jnp.tanh(z * (GELU_A + GELU_B * (z * z))))


def dot(a, b):
    return jnp.dot(a, b, preferred_element_type=jnp.float32)


def layer_kernel(
    dims,
    x_hbm, idx_hbm, gate_hbm, win_hbm, wout_hbm, sin_hbm, sout_hbm,
    y_ref,
    x_all, win, wout, idx_all, gate_all, disp, comb, rows_in, acc, hidden, rows_out,
    part, sib_part, sib_fwd, link_out, link_in, shared_h, shared_u,
    fence_sem, small_sem, x_sem, win_sem, wout_sem, shared_sem,
    meta_send, meta_recv, xl_send, xl_recv, xs_send, xs_recv, xf_send, xf_recv,
    ps_send, ps_recv, pf_send, pf_recv, pl_send, pl_recv,
):
    tok, top_k, local_e, slot, tokens = dims
    d_model, ff = win_hbm.shape[1], win_hbm.shape[2]
    chunks = d_model // COLS
    me = lax.axis_index('ep')
    chip, core = lax.div(me, 2), lax.rem(me, 2)
    sib = chip * 2 + (1 - core)
    mir = (1 - chip) * 2 + core
    diag = (1 - chip) * 2 + (1 - core)
    peers = (sib, mir, diag)

    def rows_of(dev):
        return pl.ds(pl.multiple_of(dev * tok, tok), tok)

    def remote(src, dst, send, recv, dev):
        return pltpu.make_async_remote_copy(
            src_ref=src, dst_ref=dst, send_sem=send, recv_sem=recv,
            device_id={'ep': dev}, device_id_type=MESH)

    def fence():
        pl.semaphore_signal(fence_sem, 1)
        pl.semaphore_wait(fence_sem, 1)

    idx_cp = pltpu.make_async_copy(idx_hbm, idx_all.at[me], small_sem.at[0])
    gate_cp = pltpu.make_async_copy(gate_hbm, gate_all.at[me], small_sem.at[1])
    x_cps = [pltpu.make_async_copy(x_hbm.at[:, pl.ds(k * COLS, COLS)], x_all.at[k, rows_of(me)], x_sem.at[k]) for k in range(chunks)]
    win_cps = [pltpu.make_async_copy(win_hbm.at[:, pl.ds(k * COLS, COLS), :], win.at[k], win_sem.at[k]) for k in range(chunks)]
    wout_cps = [pltpu.make_async_copy(wout_hbm.at[:, :, pl.ds(n * COLS, COLS)], wout.at[n], wout_sem.at[n]) for n in range(chunks)]
    for cp in [idx_cp, gate_cp] + x_cps:
        cp.start()

    barrier = pltpu.get_barrier_semaphore()
    for peer in peers:
        pl.semaphore_signal(barrier, inc=1, device_id={'ep': peer}, device_id_type=MESH)

    with scope('w_small'):
        for cp in [idx_cp, gate_cp] + x_cps:
            cp.wait()
    with scope('w_barrier'):
        pl.semaphore_wait(barrier, 3)
    meta_cps = []
    for r, peer in enumerate(peers):
        meta_cps.append(remote(idx_all.at[me], idx_all.at[me], meta_send.at[r], meta_recv.at[r], peer))
        meta_cps.append(remote(gate_all.at[me], gate_all.at[me], meta_send.at[3 + r], meta_recv.at[3 + r], peer))
    for cp in meta_cps:
        cp.start()
    xl_cps, xs_cps, xf_cps = [], [], []
    for k in range(chunks):
        mine, theirs = x_all.at[k, rows_of(me)], x_all.at[k, rows_of(mir)]
        xl_cps.append(remote(mine, mine, xl_send.at[k], xl_recv.at[k], mir))
        xs_cps.append(remote(mine, mine, xs_send.at[k], xs_recv.at[k], sib))
        xf_cps.append(remote(theirs, theirs, xf_send.at[k], xf_recv.at[k], sib))
    for k in range(chunks):
        xl_cps[k].start()
        xs_cps[k].start()
    for cp in win_cps + wout_cps:
        fence()
        cp.start()

    with scope('w_meta'):
        for cp in meta_cps:
            cp.wait_recv()
    group = tokens // tok
    idx_t = jnp.concatenate([idx_all[s] for s in range(group)], axis=1)
    gate_t = jnp.concatenate([gate_all[s] for s in range(group)], axis=1).astype(jnp.bfloat16).astype(jnp.float32)
    expert_id = lax.broadcasted_iota(jnp.int32, (local_e, tokens), 0) + me * local_e
    picked = jnp.zeros((local_e, tokens), jnp.float32)
    gates = jnp.zeros((local_e, tokens), jnp.float32)
    for j in range(top_k):
        hit = idx_t[j:j + 1, :] == expert_id
        picked = picked + jnp.where(hit, 1.0, 0.0)
        gates = gates + jnp.where(hit, gate_t[j:j + 1, :], 0.0)
    before = (lax.broadcasted_iota(jnp.int32, (tokens, tokens), 0) < lax.broadcasted_iota(jnp.int32, (tokens, tokens), 1))
    rank = dot(picked.astype(jnp.bfloat16), jnp.where(before, 1.0, 0.0).astype(jnp.bfloat16))
    rank = jnp.where(picked > 0.5, rank, -1.0)
    slot_id = lax.broadcasted_iota(jnp.int32, (slot, tokens), 0).astype(jnp.float32)
    for e in range(local_e):
        here = slot_id == rank[e:e + 1, :]
        disp[pl.ds(e * slot, slot), :] = jnp.where(here, 1.0, 0.0).astype(jnp.bfloat16)
        rows_out[pl.ds(e * slot, slot), :] = jnp.where(here, gates[e:e + 1, :], 0.0).astype(jnp.bfloat16)
    for i in range(local_e * slot // 256):
        comb[:, pl.ds(i * 256, 256)] = rows_out[pl.ds(i * 256, 256), :].T

    def forward(k):
        with scope(f'w_xl{k}'):
            xl_cps[k].wait_recv()
        xf_cps[k].start()

    def await_rows(k):
        with scope(f'w_xs{k}'):
            xs_cps[k].wait_recv()
        with scope(f'w_xf{k}'):
            xf_cps[k].wait_recv()

    def gather(k):
        rows_in[k % 2] = dot(disp[...], x_all[k]).astype(jnp.bfloat16)

    forward(0)
    forward(1)
    await_rows(0)
    gather(0)
    for k in range(chunks):
        if k + 2 < chunks:
            forward(k + 2)
        if k + 1 < chunks:
            await_rows(k + 1)
        with scope(f'w_win{k}'):
            win_cps[k].wait()
        if k + 1 < chunks:
            gather(k + 1)
        for e in range(local_e):
            r = pl.ds(e * slot, slot)
            term = dot(rows_in[k % 2, r, :], win[k, e])
            if k == 0:
                acc[r, :] = term
            elif k + 1 < chunks:
                acc[r, :] = acc[r, :] + term
            else:
                hidden[r, :] = gelu(acc[r, :] + term).astype(jnp.bfloat16)

    shared_cps = []
    for k in range(chunks):
        for j in range(2):
            shared_cps.append(pltpu.make_async_copy(
                sin_hbm.at[pl.ds(k * COLS, COLS), pl.ds(j * ff, ff)], win.at[k, j], shared_sem.at[k * 2 + j]))
    for i in range(4):
        for j in range(3):
            shared_cps.append(pltpu.make_async_copy(
                sout_hbm.at[pl.ds(i * COLS, COLS), pl.ds(j * ff, ff)], win.at[i, 2 + j], shared_sem.at[12 + i * 3 + j]))
    for cp in shared_cps:
        cp.start()

    ps_cps = [remote(part.at[n, rows_of(sib)], sib_part.at[n], ps_send.at[n], ps_recv.at[n], sib) for n in range(chunks)]
    pf_cps = [remote(part.at[n, rows_of(diag)], sib_fwd.at[n], pf_send.at[n], pf_recv.at[n], sib) for n in range(chunks)]
    pl_cps = [remote(link_out.at[n], link_in.at[n], pl_send.at[n], pl_recv.at[n], mir) for n in range(chunks)]

    def send_back(n):
        with scope(f'w_pf{n}'):
            pf_cps[n].wait_recv()
        link_out[n] = part[n, rows_of(mir), :] + sib_fwd[n]
        pl_cps[n].start()

    for n in range(chunks):
        with scope(f'w_wout{n}'):
            wout_cps[n].wait()
        total = None
        done = 0
        for e in range(local_e):
            r = pl.ds(e * slot, slot)
            rows_out[r, :] = dot(hidden[r, :], wout[n, e]).astype(jnp.bfloat16)
            while done + 256 <= e * slot or (e + 1 == local_e and done < local_e * slot):
                c = pl.ds(done, 256)
                term = dot(comb[:, c], rows_out[c, :])
                total = term if total is None else total + term
                done += 256
        part[n] = total
        pf_cps[n].start()
        ps_cps[n].start()
        if n:
            send_back(n - 1)
    send_back(chunks - 1)

    with scope('w_shared'):
        for cp in shared_cps:
            cp.wait()
    for j in range(2):
        s = dot(x_all[0, rows_of(me), :], win[0, j])
        for k in range(1, chunks):
            s = s + dot(x_all[k, rows_of(me), :], win[k, j])
        shared_h[:, pl.ds(j * ff, ff)] = gelu(s).astype(jnp.bfloat16)
    for j in range(3):
        u = dot(shared_h[:, 0:COLS], win[0, 2 + j])
        for i in range(1, 4):
            u = u + dot(shared_h[:, pl.ds(i * COLS, COLS)], win[i, 2 + j])
        shared_u[:, pl.ds(j * ff, ff)] = u

    for n in range(chunks):
        with scope(f'w_ps{n}'):
            ps_cps[n].wait_recv()
        mine = shared_u[:, pl.ds(n * COLS, COLS)] + part[n, rows_of(me), :] + sib_part[n]
        with scope(f'w_pl{n}'):
            pl_cps[n].wait_recv()
        y_ref[:, pl.ds(n * COLS, COLS)] = (mine + link_in[n]).astype(jnp.bfloat16)
    with scope('w_sends'):
        for cp in meta_cps + xl_cps + xs_cps + xf_cps + ps_cps + pf_cps + pl_cps:
            cp.wait_send()


def solution(mesh):
    group = mesh.shape['ep']

    def local_layer(x_loc, idx_loc, gate_loc, w_in, w_out, shared_in, shared_out):
        tok, top_k = idx_loc.shape
        local_e, d_model, ff = w_in.shape
        fs = shared_in.shape[1]
        tokens = tok * group
        cap = min(tok, LOAD_MULT * tok * top_k // (local_e * group))
        slot = -(-cap * group // 16) * 16
        total = local_e * slot
        chunks = d_model // COLS
        bf16, f32 = jnp.bfloat16, jnp.float32
        dma = pltpu.SemaphoreType.DMA
        scratch = [
            pltpu.VMEM((chunks, tokens, COLS), bf16),
            pltpu.VMEM((chunks, local_e, COLS, ff), bf16),
            pltpu.VMEM((chunks, local_e, ff, COLS), bf16),
            pltpu.VMEM((group, top_k, tok), jnp.int32),
            pltpu.VMEM((group, top_k, tok), f32),
            pltpu.VMEM((total, tokens), bf16),
            pltpu.VMEM((tokens, total), bf16),
            pltpu.VMEM((2, total, COLS), bf16),
            pltpu.VMEM((total, ff), f32),
            pltpu.VMEM((total, ff), bf16),
            pltpu.VMEM((total, COLS), bf16),
            pltpu.VMEM((chunks, tokens, COLS), f32),
            pltpu.VMEM((chunks, tok, COLS), f32),
            pltpu.VMEM((chunks, tok, COLS), f32),
            pltpu.VMEM((chunks, tok, COLS), f32),
            pltpu.VMEM((chunks, tok, COLS), f32),
            pltpu.VMEM((tok, fs), bf16),
            pltpu.VMEM((tok, d_model), f32),
            pltpu.SemaphoreType.REGULAR, dma((2,)), dma((chunks,)), dma((chunks,)), dma((chunks,)), dma((24,)),
            dma((6,)), dma((6,)),
        ] + [dma((chunks,))] * 12
        any_spec = pl.BlockSpec(memory_space=pltpu.HBM)
        return pl.pallas_call(
            functools.partial(layer_kernel, (tok, top_k, local_e, slot, tokens)),
            out_shape=pltpu.VMEM((tok, d_model), bf16),
            in_specs=[any_spec] * 7,
            out_specs=pl.BlockSpec(memory_space=pltpu.VMEM),
            scratch_shapes=scratch,
            compiler_params=pltpu.CompilerParams(
                collective_id=0, has_side_effects=True, vmem_limit_bytes=VMEM_LIMIT),
        )(x_loc, idx_loc.T, gate_loc.T, w_in, w_out, shared_in, shared_out)

    tok_spec = P(('dp', 'ep'), None)
    expert_spec = P('ep', None, None)
    whole_spec = P(None, None)
    return jax.shard_map(
        local_layer, mesh=mesh,
        in_specs=(tok_spec, tok_spec, tok_spec, expert_spec, expert_spec, whole_spec, whole_spec),
        out_specs=tok_spec, check_vma=False)
```

```python
import functools
import math

import jax
import jax.numpy as jnp
from jax import lax
from jax.experimental import pallas as pl
from jax.experimental.pallas import tpu as pltpu
from jax.sharding import PartitionSpec as P

MESH = pl.DeviceIdType.MESH
LOAD_MULT = 3
VMEM_LIMIT = 61500000
scope = jax.named_scope
COLS = 256
GELU_A = math.sqrt(2.0 / math.pi)
GELU_B = GELU_A * 0.044715


def gelu(z):
    return 0.5 * z * (1.0 + jnp.tanh(z * (GELU_A + GELU_B * (z * z))))


def dot(a, b):
    return jnp.dot(a, b, preferred_element_type=jnp.float32)


def layer_kernel(
    dims,
    x_hbm, idx_hbm, gate_hbm, win_hbm, wout_hbm, sin_hbm, sout_hbm,
    y_ref,
    x_all, win, wout, idx_all, gate_all, disp, comb, rows_in, acc, hidden, rows_out,
    part, sib_part, sib_fwd, link_out, link_in, shared_h, shared_u,
    fence_sem, small_sem, x_sem, win_sem, wout_sem, shared_sem,
    meta_send, meta_recv, xl_send, xl_recv, xs_send, xs_recv, xf_send, xf_recv,
    ps_send, ps_recv, pf_send, pf_recv, pl_send, pl_recv,
):
    tok, top_k, local_e, slot, tokens = dims
    d_model, ff = win_hbm.shape[1], win_hbm.shape[2]
    chunks = d_model // COLS
    me = lax.axis_index('ep')
    chip, core = lax.div(me, 2), lax.rem(me, 2)
    sib = chip * 2 + (1 - core)
    mir = (1 - chip) * 2 + core
    diag = (1 - chip) * 2 + (1 - core)
    peers = (sib, mir, diag)

    def rows_of(dev):
        return pl.ds(pl.multiple_of(dev * tok, tok), tok)

    def remote(src, dst, send, recv, dev):
        return pltpu.make_async_remote_copy(
            src_ref=src, dst_ref=dst, send_sem=send, recv_sem=recv,
            device_id={'ep': dev}, device_id_type=MESH)

    def fence():
        pl.semaphore_signal(fence_sem, 1)
        pl.semaphore_wait(fence_sem, 1)

    idx_cp = pltpu.make_async_copy(idx_hbm, idx_all.at[me], small_sem.at[0])
    gate_cp = pltpu.make_async_copy(gate_hbm, gate_all.at[me], small_sem.at[1])
    x_cps = [pltpu.make_async_copy(x_hbm.at[:, pl.ds(k * COLS, COLS)], x_all.at[k, rows_of(me)], x_sem.at[k]) for k in range(chunks)]
    win_cps = [pltpu.make_async_copy(win_hbm.at[:, pl.ds(k * COLS, COLS), :], win.at[k], win_sem.at[k]) for k in range(chunks)]
    wout_cps = [pltpu.make_async_copy(wout_hbm.at[:, :, pl.ds(n * COLS, COLS)], wout.at[n], wout_sem.at[n]) for n in range(chunks)]
    for cp in [idx_cp, gate_cp] + x_cps:
        cp.start()

    barrier = pltpu.get_barrier_semaphore()
    for peer in peers:
        pl.semaphore_signal(barrier, inc=1, device_id={'ep': peer}, device_id_type=MESH)

    with scope('w_small'):
        for cp in [idx_cp, gate_cp] + x_cps:
            cp.wait()
    with scope('w_barrier'):
        pl.semaphore_wait(barrier, 3)
    meta_cps = []
    for r, peer in enumerate(peers):
        meta_cps.append(remote(idx_all.at[me], idx_all.at[me], meta_send.at[r], meta_recv.at[r], peer))
        meta_cps.append(remote(gate_all.at[me], gate_all.at[me], meta_send.at[3 + r], meta_recv.at[3 + r], peer))
    for cp in meta_cps:
        cp.start()
    xl_cps, xs_cps, xf_cps = [], [], []
    for k in range(chunks):
        mine, theirs = x_all.at[k, rows_of(me)], x_all.at[k, rows_of(mir)]
        xl_cps.append(remote(mine, mine, xl_send.at[k], xl_recv.at[k], mir))
        xs_cps.append(remote(mine, mine, xs_send.at[k], xs_recv.at[k], sib))
        xf_cps.append(remote(theirs, theirs, xf_send.at[k], xf_recv.at[k], sib))
    for k in range(chunks):
        xl_cps[k].start()
        xs_cps[k].start()
    for cp in win_cps + wout_cps:
        fence()
        cp.start()

    with scope('w_meta'):
        for cp in meta_cps:
            cp.wait_recv()
    group = tokens // tok
    idx_t = jnp.concatenate([idx_all[s] for s in range(group)], axis=1)
    gate_t = jnp.concatenate([gate_all[s] for s in range(group)], axis=1).astype(jnp.bfloat16).astype(jnp.float32)
    expert_id = lax.broadcasted_iota(jnp.int32, (local_e, tokens), 0) + me * local_e
    picked = jnp.zeros((local_e, tokens), jnp.float32)
    gates = jnp.zeros((local_e, tokens), jnp.float32)
    for j in range(top_k):
        hit = idx_t[j:j + 1, :] == expert_id
        picked = picked + jnp.where(hit, 1.0, 0.0)
        gates = gates + jnp.where(hit, gate_t[j:j + 1, :], 0.0)
    before = (lax.broadcasted_iota(jnp.int32, (tokens, tokens), 0) < lax.broadcasted_iota(jnp.int32, (tokens, tokens), 1))
    rank = dot(picked.astype(jnp.bfloat16), jnp.where(before, 1.0, 0.0).astype(jnp.bfloat16))
    rank = jnp.where(picked > 0.5, rank, -1.0)
    slot_id = lax.broadcasted_iota(jnp.int32, (slot, tokens), 0).astype(jnp.float32)
    for e in range(local_e):
        here = slot_id == rank[e:e + 1, :]
        disp[pl.ds(e * slot, slot), :] = jnp.where(here, 1.0, 0.0).astype(jnp.bfloat16)
        rows_out[pl.ds(e * slot, slot), :] = jnp.where(here, gates[e:e + 1, :], 0.0).astype(jnp.bfloat16)
    for i in range(local_e * slot // 256):
        comb[:, pl.ds(i * 256, 256)] = rows_out[pl.ds(i * 256, 256), :].T

    def forward(k):
        with scope(f'w_xl{k}'):
            xl_cps[k].wait_recv()
        xf_cps[k].start()

    def await_rows(k):
        with scope(f'w_xs{k}'):
            xs_cps[k].wait_recv()
        with scope(f'w_xf{k}'):
            xf_cps[k].wait_recv()

    def gather(k, piece, pieces):
        m = local_e * slot // pieces
        r = pl.ds(piece * m, m)
        rows_in[k % 2, r, :] = dot(disp[r, :], x_all[k]).astype(jnp.bfloat16)

    forward(0)
    forward(1)
    await_rows(0)
    gather(0, 0, 2)
    gather(0, 1, 2)
    for k in range(chunks):
        if k + 2 < chunks:
            forward(k + 2)
        if k + 1 < chunks:
            await_rows(k + 1)
        with scope(f'w_win{k}'):
            win_cps[k].wait()
        if k + 1 == chunks:
            with scope('w_wout0'):
                wout_cps[0].wait()
        for e in range(local_e):
            r = pl.ds(e * slot, slot)
            for h in range(1):
                c = pl.ds(h * (ff // 1), ff // 1)
                term = dot(rows_in[k % 2, r, :], win[k, e, :, c])
                if k == 0:
                    acc[r, c] = term
                elif k + 1 < chunks:
                    acc[r, c] = acc[r, c] + term
                else:
                    hidden[r, c] = gelu(acc[r, c] + term).astype(jnp.bfloat16)
            if k + 1 < chunks and e in [0,2,4,6,8,10,12,13]:
                gather(k + 1, [0,2,4,6,8,10,12,13].index(e), len([0,2,4,6,8,10,12,13]))

    shared_cps = []

    def load_shared():
        for k in range(chunks):
            for j in range(2):
                shared_cps.append(pltpu.make_async_copy(
                    sin_hbm.at[pl.ds(k * COLS, COLS), pl.ds(j * ff, ff)], win.at[k, j], shared_sem.at[k * 2 + j]))
        for i in range(4):
            for j in range(3):
                shared_cps.append(pltpu.make_async_copy(
                    sout_hbm.at[pl.ds(i * COLS, COLS), pl.ds(j * ff, ff)], win.at[i, 2 + j], shared_sem.at[12 + i * 3 + j]))
        for cp in shared_cps:
            cp.start()

    ps_cps = [remote(part.at[n, rows_of(sib)], sib_part.at[n], ps_send.at[n], ps_recv.at[n], sib) for n in range(chunks)]
    pf_cps = [remote(part.at[n, rows_of(diag)], sib_fwd.at[n], pf_send.at[n], pf_recv.at[n], sib) for n in range(chunks)]
    pl_cps = [remote(link_out.at[n], link_in.at[n], pl_send.at[n], pl_recv.at[n], mir) for n in range(chunks)]

    def send_back(n):
        with scope(f'w_pf{n}'):
            pf_cps[n].wait_recv()
        link_out[n] = part[n, rows_of(mir), :] + sib_fwd[n]
        pl_cps[n].start()

    for n in range(chunks):
        if n:
            with scope(f'w_wout{n}'):
                wout_cps[n].wait()
        total = None
        done = 0
        for e in range(local_e):
            r = pl.ds(e * slot, slot)
            rows_out[r, :] = dot(hidden[r, :], wout[n, e]).astype(jnp.bfloat16)
            while done + 256 <= e * slot or (e + 1 == local_e and done < local_e * slot):
                c = pl.ds(done, 256)
                term = dot(comb[:, c], rows_out[c, :])
                total = term if total is None else total + term
                done += 256
        part[n] = total
        pf_cps[n].start()
        ps_cps[n].start()
        if n == 0:
            load_shared()
        if n:
            send_back(n - 1)
    send_back(chunks - 1)

    with scope('w_shared'):
        for cp in shared_cps:
            cp.wait()
    for j in range(2):
        s = dot(x_all[0, rows_of(me), :], win[0, j])
        for k in range(1, chunks):
            s = s + dot(x_all[k, rows_of(me), :], win[k, j])
        shared_h[:, pl.ds(j * ff, ff)] = gelu(s).astype(jnp.bfloat16)
    for j in range(3):
        u = dot(shared_h[:, 0:COLS], win[0, 2 + j])
        for i in range(1, 4):
            u = u + dot(shared_h[:, pl.ds(i * COLS, COLS)], win[i, 2 + j])
        shared_u[:, pl.ds(j * ff, ff)] = u

    for n in range(chunks):
        with scope(f'w_ps{n}'):
            ps_cps[n].wait_recv()
        mine = shared_u[:, pl.ds(n * COLS, COLS)] + part[n, rows_of(me), :] + sib_part[n]
        with scope(f'w_pl{n}'):
            pl_cps[n].wait_recv()
        y_ref[:, pl.ds(n * COLS, COLS)] = (mine + link_in[n]).astype(jnp.bfloat16)
    with scope('w_sends'):
        for cp in meta_cps + xl_cps + xs_cps + xf_cps + ps_cps + pf_cps + pl_cps:
            cp.wait_send()


def solution(mesh):
    group = mesh.shape['ep']

    def local_layer(x_loc, idx_loc, gate_loc, w_in, w_out, shared_in, shared_out):
        tok, top_k = idx_loc.shape
        local_e, d_model, ff = w_in.shape
        fs = shared_in.shape[1]
        tokens = tok * group
        cap = min(tok, LOAD_MULT * tok * top_k // (local_e * group))
        slot = -(-cap * group // 16) * 16
        total = local_e * slot
        chunks = d_model // COLS
        bf16, f32 = jnp.bfloat16, jnp.float32
        dma = pltpu.SemaphoreType.DMA
        scratch = [
            pltpu.VMEM((chunks, tokens, COLS), bf16),
            pltpu.VMEM((chunks, local_e, COLS, ff), bf16),
            pltpu.VMEM((chunks, local_e, ff, COLS), bf16),
            pltpu.VMEM((group, top_k, tok), jnp.int32),
            pltpu.VMEM((group, top_k, tok), f32),
            pltpu.VMEM((total, tokens), bf16),
            pltpu.VMEM((tokens, total), bf16),
            pltpu.VMEM((2, total, COLS), bf16),
            pltpu.VMEM((total, ff), f32),
            pltpu.VMEM((total, ff), bf16),
            pltpu.VMEM((total, COLS), bf16),
            pltpu.VMEM((chunks, tokens, COLS), f32),
            pltpu.VMEM((chunks, tok, COLS), f32),
            pltpu.VMEM((chunks, tok, COLS), f32),
            pltpu.VMEM((chunks, tok, COLS), f32),
            pltpu.VMEM((chunks, tok, COLS), f32),
            pltpu.VMEM((tok, fs), bf16),
            pltpu.VMEM((tok, d_model), f32),
            pltpu.SemaphoreType.REGULAR, dma((2,)), dma((chunks,)), dma((chunks,)), dma((chunks,)), dma((24,)),
            dma((6,)), dma((6,)),
        ] + [dma((chunks,))] * 12
        any_spec = pl.BlockSpec(memory_space=pltpu.HBM)
        return pl.pallas_call(
            functools.partial(layer_kernel, (tok, top_k, local_e, slot, tokens)),
            out_shape=pltpu.VMEM((tok, d_model), bf16),
            in_specs=[any_spec] * 7,
            out_specs=pl.BlockSpec(memory_space=pltpu.VMEM),
            scratch_shapes=scratch,
            compiler_params=pltpu.CompilerParams(
                collective_id=0, has_side_effects=True, vmem_limit_bytes=VMEM_LIMIT),
        )(x_loc, idx_loc.T, gate_loc.T, w_in, w_out, shared_in, shared_out)

    tok_spec = P(('dp', 'ep'), None)
    expert_spec = P('ep', None, None)
    whole_spec = P(None, None)
    return jax.shard_map(
        local_layer, mesh=mesh,
        in_specs=(tok_spec, tok_spec, tok_spec, expert_spec, expert_spec, whole_spec, whole_spec),
        out_specs=tok_spec, check_vma=False)
```

```python
import functools
import math

import jax
import jax.numpy as jnp
from jax import lax
from jax.experimental import pallas as pl
from jax.experimental.pallas import tpu as pltpu
from jax.sharding import PartitionSpec as P

MESH = pl.DeviceIdType.MESH
LOAD_MULT = 3
SPOTS = (0, 2, 4, 6, 8, 10, 12, 13)
LAG = 2
VMEM_LIMIT = 61500000
scope = jax.named_scope
COLS = 256
GELU_A = math.sqrt(2.0 / math.pi)
GELU_B = GELU_A * 0.044715


def gelu(z):
    return 0.5 * z * (1.0 + jnp.tanh(z * (GELU_A + GELU_B * (z * z))))


def dot(a, b):
    return jnp.dot(a, b, preferred_element_type=jnp.float32)


def layer_kernel(
    dims,
    x_hbm, idx_hbm, gate_hbm, win_hbm, wout_hbm, sin_hbm, sout_hbm,
    y_ref,
    x_all, win, wout, idx_all, gate_all, disp, comb, rows_in, acc, hidden, rows_out,
    part, sib_part, sib_fwd, link_out, link_in, shared_h, shared_u,
    *sems):
    (fence_sem, small_sem, x_sem, win_sem, wout_sem, shared_sem,
     meta_send, meta_recv, xl_send, xl_recv, xs_send, xs_recv, xf_send, xf_recv,
     ps_send, ps_recv, pf_send, pf_recv, pl_send, pl_recv) = sems
    tok, top_k, local_e, slot, tokens = dims
    d_model, ff = win_hbm.shape[1], win_hbm.shape[2]
    chunks = d_model // COLS
    me = lax.axis_index('ep')
    chip, core = lax.div(me, 2), lax.rem(me, 2)
    sib = chip * 2 + (1 - core)
    mir = (1 - chip) * 2 + core
    diag = (1 - chip) * 2 + (1 - core)
    peers = (sib, mir, diag)

    def rows_of(dev):
        return pl.ds(pl.multiple_of(dev * tok, tok), tok)

    def remote(src, dst, send, recv, dev):
        return pltpu.make_async_remote_copy(
            src_ref=src, dst_ref=dst, send_sem=send, recv_sem=recv,
            device_id={'ep': dev}, device_id_type=MESH)

    def fence():
        pl.semaphore_signal(fence_sem, 1)
        pl.semaphore_wait(fence_sem, 1)

    idx_cp = pltpu.make_async_copy(idx_hbm, idx_all.at[me], small_sem.at[0])
    gate_cp = pltpu.make_async_copy(gate_hbm, gate_all.at[me], small_sem.at[1])
    x_cps = [pltpu.make_async_copy(x_hbm.at[:, pl.ds(k * COLS, COLS)], x_all.at[k, rows_of(me)], x_sem.at[k]) for k in range(chunks)]
    win_cps = [pltpu.make_async_copy(win_hbm.at[:, pl.ds(k * COLS, COLS), :], win.at[k], win_sem.at[k]) for k in range(chunks)]
    wout_cps = [pltpu.make_async_copy(wout_hbm.at[:, :, pl.ds(n * COLS, COLS)], wout.at[n], wout_sem.at[n]) for n in range(chunks)]
    for cp in [idx_cp, gate_cp] + x_cps:
        cp.start()

    barrier = pltpu.get_barrier_semaphore()
    for peer in peers:
        pl.semaphore_signal(barrier, inc=1, device_id={'ep': peer}, device_id_type=MESH)

    with scope('w_small'):
        for cp in [idx_cp, gate_cp] + x_cps:
            cp.wait()
    with scope('w_barrier'):
        pl.semaphore_wait(barrier, 3)
    meta_cps = []
    for r, peer in enumerate(peers):
        meta_cps.append(remote(idx_all.at[me], idx_all.at[me], meta_send.at[r], meta_recv.at[r], peer))
        meta_cps.append(remote(gate_all.at[me], gate_all.at[me], meta_send.at[3 + r], meta_recv.at[3 + r], peer))
    for cp in meta_cps:
        cp.start()
    xl_cps, xs_cps, xf_cps = [], [], []
    for k in range(chunks):
        mine, theirs = x_all.at[k, rows_of(me)], x_all.at[k, rows_of(mir)]
        xl_cps.append(remote(mine, mine, xl_send.at[k], xl_recv.at[k], mir))
        xs_cps.append(remote(mine, mine, xs_send.at[k], xs_recv.at[k], sib))
        xf_cps.append(remote(theirs, theirs, xf_send.at[k], xf_recv.at[k], sib))
    for k in range(chunks):
        xl_cps[k].start()
        xs_cps[k].start()
    for cp in win_cps + wout_cps:
        fence()
        cp.start()

    with scope('w_meta'):
        for cp in meta_cps:
            cp.wait_recv()
    group = tokens // tok
    idx_t = jnp.concatenate([idx_all[s] for s in range(group)], axis=1)
    gate_t = jnp.concatenate([gate_all[s] for s in range(group)], axis=1).astype(jnp.bfloat16).astype(jnp.float32)
    expert_id = lax.broadcasted_iota(jnp.int32, (local_e, tokens), 0) + me * local_e
    picked = jnp.zeros((local_e, tokens), jnp.float32)
    gates = jnp.zeros((local_e, tokens), jnp.float32)
    for j in range(top_k):
        hit = idx_t[j:j + 1, :] == expert_id
        picked = picked + jnp.where(hit, 1.0, 0.0)
        gates = gates + jnp.where(hit, gate_t[j:j + 1, :], 0.0)
    before = (lax.broadcasted_iota(jnp.int32, (tokens, tokens), 0) < lax.broadcasted_iota(jnp.int32, (tokens, tokens), 1))
    rank = dot(picked.astype(jnp.bfloat16), jnp.where(before, 1.0, 0.0).astype(jnp.bfloat16))
    rank = jnp.where(picked > 0.5, rank, -1.0)
    slot_id = lax.broadcasted_iota(jnp.int32, (slot, tokens), 0).astype(jnp.float32)
    for e in range(local_e):
        here = slot_id == rank[e:e + 1, :]
        disp[pl.ds(e * slot, slot), :] = jnp.where(here, 1.0, 0.0).astype(jnp.bfloat16)
        rows_out[pl.ds(e * slot, slot), :] = jnp.where(here, gates[e:e + 1, :], 0.0).astype(jnp.bfloat16)
    for i in range(local_e * slot // 256):
        comb[:, pl.ds(i * 256, 256)] = rows_out[pl.ds(i * 256, 256), :].T

    def forward(k):
        with scope(f'w_xl{k}'):
            xl_cps[k].wait_recv()
        xf_cps[k].start()

    def await_rows(k):
        with scope(f'w_xs{k}'):
            xs_cps[k].wait_recv()
        with scope(f'w_xf{k}'):
            xf_cps[k].wait_recv()

    def gather(k, piece, pieces):
        m = local_e * slot // pieces
        r = pl.ds(piece * m, m)
        rows_in[k % 2, r, :] = dot(disp[r, :], x_all[k]).astype(jnp.bfloat16)

    forward(0)
    forward(1)
    await_rows(0)
    gather(0, 0, 2)
    gather(0, 1, 2)
    def first(k, e):
        r = pl.ds(e * slot, slot)
        term = dot(rows_in[k % 2, r, :], win[k, e])
        if k == 0:
            acc[r, :] = term
        elif k + 1 < chunks:
            acc[r, :] = acc[r, :] + term
        else:
            hidden[r, :] = gelu(acc[r, :] + term).astype(jnp.bfloat16)

    def second(n, e, total):
        r = pl.ds(e * slot, slot)
        rows_out[r, :] = dot(hidden[r, :], wout[n, e]).astype(jnp.bfloat16)
        ready = e * slot // COLS if e + 1 < local_e else local_e * slot // COLS
        for i in range(max(e - 1, 0) * slot // COLS, ready):
            c = pl.ds(i * COLS, COLS)
            term = dot(comb[:, c], rows_out[c, :])
            total = term if total is None else total + term
        return total

    for k in range(chunks):
        if k + 2 < chunks:
            forward(k + 2)
        if k + 1 < chunks:
            await_rows(k + 1)
        with scope(f'w_win{k}'):
            win_cps[k].wait()
        if k + 1 < chunks:
            for e in range(local_e):
                first(k, e)
                if e in SPOTS:
                    gather(k + 1, SPOTS.index(e), len(SPOTS))
    with scope('w_wout0'):
        wout_cps[0].wait()
    total = None
    for e in range(local_e + LAG):
        if e < local_e:
            first(chunks - 1, e)
        if e >= LAG:
            total = second(0, e - LAG, total)

    shared_cps = []

    def load_shared():
        for j in range(2):
            shared_cps.append(pltpu.make_async_copy(sin_hbm.at[:, :, pl.ds(j * ff, ff)], win.at[:, j], shared_sem.at[j]))
        for j in range(3):
            shared_cps.append(pltpu.make_async_copy(
                sout_hbm.at[:, :, pl.ds(j * ff, ff)], win.at[pl.ds(0, sout_hbm.shape[0]), 2 + j], shared_sem.at[2 + j]))
        for cp in shared_cps:
            cp.start()

    ps_cps = [remote(part.at[n, rows_of(sib)], sib_part.at[n], ps_send.at[n], ps_recv.at[n], sib) for n in range(chunks)]
    pf_cps = [remote(part.at[n, rows_of(diag)], sib_fwd.at[n], pf_send.at[n], pf_recv.at[n], sib) for n in range(chunks)]
    pl_cps = [remote(link_out.at[n], link_in.at[n], pl_send.at[n], pl_recv.at[n], mir) for n in range(chunks)]

    def send_back(n):
        with scope(f'w_pf{n}'):
            pf_cps[n].wait_recv()
        link_out[n] = part[n, rows_of(mir), :] + sib_fwd[n]
        pl_cps[n].start()

    for n in range(chunks):
        if n:
            with scope(f'w_wout{n}'):
                wout_cps[n].wait()
        if n:
            total = None
            for e in range(local_e):
                total = second(n, e, total)
        part[n] = total
        pf_cps[n].start()
        ps_cps[n].start()
        if n == 0:
            load_shared()
        if n:
            send_back(n - 1)
    send_back(chunks - 1)

    with scope('w_shared'):
        for cp in shared_cps:
            cp.wait()
    for j in range(2):
        s = dot(x_all[0, rows_of(me), :], win[0, j])
        for k in range(1, chunks):
            s = s + dot(x_all[k, rows_of(me), :], win[k, j])
        shared_h[:, pl.ds(j * ff, ff)] = gelu(s).astype(jnp.bfloat16)
    for j in range(3):
        u = dot(shared_h[:, 0:COLS], win[0, 2 + j])
        for i in range(1, 4):
            u = u + dot(shared_h[:, pl.ds(i * COLS, COLS)], win[i, 2 + j])
        shared_u[:, pl.ds(j * ff, ff)] = u

    for n in range(chunks):
        with scope(f'w_ps{n}'):
            ps_cps[n].wait_recv()
        mine = shared_u[:, pl.ds(n * COLS, COLS)] + part[n, rows_of(me), :] + sib_part[n]
        with scope(f'w_pl{n}'):
            pl_cps[n].wait_recv()
        y_ref[:, pl.ds(n * COLS, COLS)] = (mine + link_in[n]).astype(jnp.bfloat16)
    with scope('w_sends'):
        for cp in meta_cps + xl_cps + xs_cps + xf_cps + ps_cps + pf_cps + pl_cps:
            cp.wait_send()


def solution(mesh):
    group = mesh.shape['ep']

    def local_layer(x_loc, idx_loc, gate_loc, w_in, w_out, shared_in, shared_out):
        tok, top_k = idx_loc.shape
        local_e, d_model, ff = w_in.shape
        fs = shared_in.shape[1]
        tokens = tok * group
        cap = min(tok, LOAD_MULT * tok * top_k // (local_e * group))
        slot = -(-cap * group // 16) * 16
        total = local_e * slot
        chunks = d_model // COLS
        bf16, f32 = jnp.bfloat16, jnp.float32
        dma = pltpu.SemaphoreType.DMA
        scratch = [
            pltpu.VMEM((chunks, tokens, COLS), bf16),
            pltpu.VMEM((chunks, local_e, COLS, ff), bf16),
            pltpu.VMEM((chunks, local_e, ff, COLS), bf16),
            pltpu.VMEM((group, top_k, tok), jnp.int32),
            pltpu.VMEM((group, top_k, tok), f32),
            pltpu.VMEM((total, tokens), bf16),
            pltpu.VMEM((tokens, total), bf16),
            pltpu.VMEM((2, total, COLS), bf16),
            pltpu.VMEM((total, ff), f32),
            pltpu.VMEM((total, ff), bf16),
            pltpu.VMEM((total, COLS), bf16),
            pltpu.VMEM((chunks, tokens, COLS), f32),
            pltpu.VMEM((chunks, tok, COLS), f32),
            pltpu.VMEM((chunks, tok, COLS), f32),
            pltpu.VMEM((chunks, tok, COLS), f32),
            pltpu.VMEM((chunks, tok, COLS), f32),
            pltpu.VMEM((tok, fs), bf16),
            pltpu.VMEM((tok, d_model), f32),
        ]
        sems = [pltpu.SemaphoreType.REGULAR, dma((2,)), dma((chunks,)), dma((chunks,)), dma((chunks,)), dma((5,)), dma((6,)), dma((6,))]
        sems += [dma((chunks,))] * 12

        def kernel(*refs):
            pl.run_scoped(functools.partial(layer_kernel, (tok, top_k, local_e, slot, tokens), *refs), *sems)

        any_spec = pl.BlockSpec(memory_space=pltpu.HBM)
        return pl.pallas_call(
            kernel,
            out_shape=pltpu.VMEM((tok, d_model), bf16),
            in_specs=[any_spec] * 7,
            out_specs=pl.BlockSpec(memory_space=pltpu.VMEM),
            scratch_shapes=scratch,
            compiler_params=pltpu.CompilerParams(
                collective_id=0, has_side_effects=True, vmem_limit_bytes=VMEM_LIMIT),
        )(x_loc, idx_loc.T, gate_loc.T, w_in, w_out,
          shared_in.reshape(chunks, COLS, fs), shared_out.reshape(fs // COLS, COLS, d_model))

    tok_spec = P(('dp', 'ep'), None)
    expert_spec = P('ep', None, None)
    whole_spec = P(None, None)
    return jax.shard_map(
        local_layer, mesh=mesh,
        in_specs=(tok_spec, tok_spec, tok_spec, expert_spec, expert_spec, whole_spec, whole_spec),
        out_specs=tok_spec, check_vma=False)
```

```python
import functools
import math

import jax
import jax.numpy as jnp
from jax import lax
from jax.experimental import pallas as pl
from jax.experimental.pallas import tpu as pltpu
from jax.sharding import PartitionSpec as P

MESH = pl.DeviceIdType.MESH
LOAD_MULT = 3
SPOTS = (0, 2, 4, 6, 8, 10, 12, 13)
DIRECT = 128
EARLY = 12
LAG = 2
VMEM_LIMIT = 62500000
scope = jax.named_scope
COLS = 256
GELU_A = math.sqrt(2.0 / math.pi)
GELU_B = GELU_A * 0.044715


def gelu(z):
    return 0.5 * z * (1.0 + jnp.tanh(z * (GELU_A + GELU_B * (z * z))))


def dot(a, b):
    return jnp.dot(a, b, preferred_element_type=jnp.float32)


def layer_kernel(
    dims,
    x_hbm, idx_hbm, gate_hbm, win_hbm, wout_hbm, sin_hbm, sout_hbm,
    y_ref,
    x_all, win, wout, idx_all, gate_all, disp, comb, rows_in, acc, hidden, rows_out,
    part, sib_part, sib_fwd, link_out, link_in, direct_a, direct_b, shared_h, shared_u,
    *sems):
    (fence_sem, small_sem, x_sem, win_sem, wout_sem, shared_sem,
     meta_send, meta_recv, xl_send, xl_recv, xs_send, xs_recv, xf_send, xf_recv,
     ps_send, ps_recv, pf_send, pf_recv, pl_send, pl_recv, direct_send, direct_recv) = sems
    tok, top_k, local_e, slot, tokens = dims
    d_model, ff = win_hbm.shape[1], win_hbm.shape[2]
    chunks = d_model // COLS
    me = lax.axis_index('ep')
    chip, core = lax.div(me, 2), lax.rem(me, 2)
    sib = chip * 2 + (1 - core)
    partner = (1 - chip) * 2 + (1 - core)
    other = (1 - chip) * 2 + core
    peers = (sib, partner, other)

    def rows_of(dev):
        return pl.ds(pl.multiple_of(dev * tok, tok), tok)

    def remote(src, dst, send, recv, dev):
        return pltpu.make_async_remote_copy(
            src_ref=src, dst_ref=dst, send_sem=send, recv_sem=recv,
            device_id={'ep': dev}, device_id_type=MESH)

    def fence():
        pl.semaphore_signal(fence_sem, 1)
        pl.semaphore_wait(fence_sem, 1)

    idx_cp = pltpu.make_async_copy(idx_hbm, idx_all.at[me], small_sem.at[0])
    gate_cp = pltpu.make_async_copy(gate_hbm, gate_all.at[me], small_sem.at[1])
    x_cps = [pltpu.make_async_copy(x_hbm.at[:, pl.ds(k * COLS, COLS)], x_all.at[k, rows_of(me)], x_sem.at[k]) for k in range(chunks)]
    win_cps = [pltpu.make_async_copy(win_hbm.at[:, pl.ds(k * COLS, COLS), :], win.at[k], win_sem.at[k]) for k in range(chunks)]
    wout_cps = [pltpu.make_async_copy(wout_hbm.at[:, :, pl.ds(n * COLS, COLS)], wout.at[n], wout_sem.at[n]) for n in range(chunks)]
    barrier = pltpu.get_barrier_semaphore()
    for peer in peers:
        pl.semaphore_signal(barrier, inc=1, device_id={'ep': peer}, device_id_type=MESH)
    for cp in [idx_cp, gate_cp] + x_cps:
        cp.start()
    for cp in win_cps + wout_cps:
        fence()
        cp.start()

    with scope('w_small'):
        for cp in [idx_cp, gate_cp] + x_cps:
            cp.wait()
    with scope('w_barrier'):
        pl.semaphore_wait(barrier, 3)
    meta_cps = []
    for r, peer in enumerate(peers):
        meta_cps.append(remote(idx_all.at[me], idx_all.at[me], meta_send.at[r], meta_recv.at[r], peer))
        meta_cps.append(remote(gate_all.at[me], gate_all.at[me], meta_send.at[3 + r], meta_recv.at[3 + r], peer))
    for cp in meta_cps:
        cp.start()
    xl_cps, xs_cps, xf_cps = [], [], []
    for k in range(chunks):
        mine, theirs = x_all.at[k, rows_of(me)], x_all.at[k, rows_of(partner)]
        xl_cps.append(remote(mine, mine, xl_send.at[k], xl_recv.at[k], partner))
        xs_cps.append(remote(mine, mine, xs_send.at[k], xs_recv.at[k], sib))
        xf_cps.append(remote(theirs, theirs, xf_send.at[k], xf_recv.at[k], sib))
    for k in range(chunks):
        xl_cps[k].start()
        xs_cps[k].start()

    with scope('w_meta'):
        for cp in meta_cps:
            cp.wait_recv()
    group = tokens // tok
    idx_t = jnp.concatenate([idx_all[s] for s in range(group)], axis=1)
    gate_t = jnp.concatenate([gate_all[s] for s in range(group)], axis=1).astype(jnp.bfloat16).astype(jnp.float32)
    expert_id = lax.broadcasted_iota(jnp.int32, (local_e, tokens), 0) + me * local_e
    picked = jnp.zeros((local_e, tokens), jnp.float32)
    gates = jnp.zeros((local_e, tokens), jnp.float32)
    for j in range(top_k):
        hit = idx_t[j:j + 1, :] == expert_id
        picked = picked + jnp.where(hit, 1.0, 0.0)
        gates = gates + jnp.where(hit, gate_t[j:j + 1, :], 0.0)
    before = (lax.broadcasted_iota(jnp.int32, (tokens, tokens), 0) < lax.broadcasted_iota(jnp.int32, (tokens, tokens), 1))
    rank = dot(picked.astype(jnp.bfloat16), jnp.where(before, 1.0, 0.0).astype(jnp.bfloat16))
    rank = jnp.where(picked > 0.5, rank, -1.0)
    slot_id = lax.broadcasted_iota(jnp.int32, (slot, tokens), 0).astype(jnp.float32)
    for e in range(local_e):
        here = slot_id == rank[e:e + 1, :]
        disp[pl.ds(e * slot, slot), :] = jnp.where(here, 1.0, 0.0).astype(jnp.bfloat16)
        rows_out[pl.ds(e * slot, slot), :] = jnp.where(here, gates[e:e + 1, :], 0.0).astype(jnp.bfloat16)
    for i in range(local_e * slot // 256):
        comb[:, pl.ds(i * 256, 256)] = rows_out[pl.ds(i * 256, 256), :].T

    def forward(k):
        with scope(f'w_xl{k}'):
            xl_cps[k].wait_recv()
        xf_cps[k].start()

    def await_rows(k):
        with scope(f'w_xs{k}'):
            xs_cps[k].wait_recv()
        with scope(f'w_xf{k}'):
            xf_cps[k].wait_recv()

    def gather(k, piece, pieces):
        m = local_e * slot // pieces
        r = pl.ds(piece * m, m)
        rows_in[k % 3, r, :] = dot(disp[r, :], x_all[k]).astype(jnp.bfloat16)

    forward(0)
    forward(1)
    await_rows(0)
    gather(0, 0, 2)
    gather(0, 1, 2)
    def first(k, e):
        r = pl.ds(e * slot, slot)
        term = dot(rows_in[k % 3, r, :], win[k, e])
        if k == 0:
            acc[r, :] = term
        elif k + 2 < chunks:
            acc[r, :] = acc[r, :] + term
        else:
            term = term + dot(rows_in[(k + 1) % 3, r, :], win[k + 1, e])
            hidden[r, :] = gelu(acc[r, :] + term).astype(jnp.bfloat16)

    def second(n, e, total):
        r = pl.ds(e * slot, slot)
        rows_out[r, :] = dot(hidden[r, :], wout[n, e]).astype(jnp.bfloat16)
        ready = e * slot // COLS if e + 1 < local_e else local_e * slot // COLS
        for i in range(max(e - 1, 0) * slot // COLS, ready):
            c = pl.ds(i * COLS, COLS)
            term = dot(comb[:, c], rows_out[c, :])
            total = term if total is None else total + term
        return total

    for k in range(chunks - 2):
        if k + 3 < chunks:
            forward(k + 2)
        await_rows(k + 1)
        if k + 4 == chunks:
            forward(chunks - 1)
        if k + 3 == chunks:
            await_rows(chunks - 1)
        with scope(f'w_win{k}'):
            win_cps[k].wait()
        for e in range(local_e):
            first(k, e)
            if e in SPOTS:
                gather(k + 1, SPOTS.index(e), len(SPOTS))
                if k + 3 == chunks:
                    gather(chunks - 1, SPOTS.index(e), len(SPOTS))
    for k in range(chunks - 2, chunks):
        with scope(f'w_win{k}'):
            win_cps[k].wait()
    with scope('w_wout0'):
        wout_cps[0].wait()
    total = None
    for e in range(local_e + LAG):
        if e < local_e:
            first(chunks - 2, e)
        if e >= LAG:
            total = second(0, e - LAG, total)

    shared_cps = []

    def load_shared():
        for j in range(2):
            shared_cps.append(pltpu.make_async_copy(sin_hbm.at[:, :, pl.ds(j * ff, ff)], win.at[:, j], shared_sem.at[j]))
        for j in range(3):
            shared_cps.append(pltpu.make_async_copy(
                sout_hbm.at[:, :, pl.ds(j * ff, ff)], win.at[pl.ds(0, sout_hbm.shape[0]), 2 + j], shared_sem.at[2 + j]))
        for cp in shared_cps:
            cp.start()

    head, rest = pl.ds(0, DIRECT), pl.ds(DIRECT, COLS - DIRECT)
    da_cp = remote(part.at[0, rows_of(partner), head], direct_a, direct_send.at[0], direct_recv.at[0], partner)
    db_cp = remote(part.at[0, rows_of(other), head], direct_b, direct_send.at[1], direct_recv.at[1], other)
    ps_cps = [remote(part.at[n, rows_of(sib)], sib_part.at[n], ps_send.at[n], ps_recv.at[n], sib) for n in range(chunks)]
    pf_cps = [remote(part.at[0, rows_of(other), rest], sib_fwd.at[0, :, rest], pf_send.at[0], pf_recv.at[0], sib)]
    pl_cps = [remote(link_out.at[0, :, rest], link_in.at[0, :, rest], pl_send.at[0], pl_recv.at[0], partner)]
    for n in range(1, chunks):
        pf_cps.append(remote(part.at[n, rows_of(other)], sib_fwd.at[n], pf_send.at[n], pf_recv.at[n], sib))
        pl_cps.append(remote(link_out.at[n], link_in.at[n], pl_send.at[n], pl_recv.at[n], partner))

    def send_back(n):
        with scope(f'w_pf{n}'):
            pf_cps[n].wait_recv()
        c = pl.ds(0, COLS) if n else rest
        link_out[n, :, c] = part[n, rows_of(partner), c] + sib_fwd[n, :, c]
        pl_cps[n].start()

    for n in range(chunks):
        if n:
            with scope(f'w_wout{n}'):
                wout_cps[n].wait()
        if n:
            total = None
            for e in range(local_e):
                if n == 1 and e == EARLY:
                    send_back(0)
                total = second(n, e, total)
        part[n] = total
        pf_cps[n].start()
        if n == 0:
            da_cp.start()
            db_cp.start()
        ps_cps[n].start()
        if n == 0:
            load_shared()
        if n > 1:
            send_back(n - 1)
    send_back(chunks - 1)

    with scope('w_shared'):
        for cp in shared_cps:
            cp.wait()
    for j in range(2):
        s = dot(x_all[0, rows_of(me), :], win[0, j])
        for k in range(1, chunks):
            s = s + dot(x_all[k, rows_of(me), :], win[k, j])
        shared_h[:, pl.ds(j * ff, ff)] = gelu(s).astype(jnp.bfloat16)
    for j in range(3):
        u = dot(shared_h[:, 0:COLS], win[0, 2 + j])
        for i in range(1, 4):
            u = u + dot(shared_h[:, pl.ds(i * COLS, COLS)], win[i, 2 + j])
        shared_u[:, pl.ds(j * ff, ff)] = u

    for n in range(chunks):
        with scope(f'w_ps{n}'):
            ps_cps[n].wait_recv()
        mine = shared_u[:, pl.ds(n * COLS, COLS)] + part[n, rows_of(me), :] + sib_part[n]
        with scope(f'w_pl{n}'):
            pl_cps[n].wait_recv()
        if n:
            y_ref[:, pl.ds(n * COLS, COLS)] = (mine + link_in[n]).astype(jnp.bfloat16)
        else:
            da_cp.wait_recv()
            db_cp.wait_recv()
            y_ref[:, head] = (mine[:, :DIRECT] + (direct_a[...] + direct_b[...])).astype(jnp.bfloat16)
            y_ref[:, rest] = (mine[:, DIRECT:] + link_in[0, :, rest]).astype(jnp.bfloat16)
    with scope('w_sends'):
        for cp in [da_cp, db_cp] + meta_cps + xl_cps + xs_cps + xf_cps + ps_cps + pf_cps + pl_cps:
            cp.wait_send()


def solution(mesh):
    group = mesh.shape['ep']

    def local_layer(x_loc, idx_loc, gate_loc, w_in, w_out, shared_in, shared_out):
        tok, top_k = idx_loc.shape
        local_e, d_model, ff = w_in.shape
        fs = shared_in.shape[1]
        tokens = tok * group
        cap = min(tok, LOAD_MULT * tok * top_k // (local_e * group))
        slot = -(-cap * group // 16) * 16
        total = local_e * slot
        chunks = d_model // COLS
        bf16, f32 = jnp.bfloat16, jnp.float32
        dma = pltpu.SemaphoreType.DMA
        scratch = [
            pltpu.VMEM((chunks, tokens, COLS), bf16),
            pltpu.VMEM((chunks, local_e, COLS, ff), bf16),
            pltpu.VMEM((chunks, local_e, ff, COLS), bf16),
            pltpu.VMEM((group, top_k, tok), jnp.int32),
            pltpu.VMEM((group, top_k, tok), f32),
            pltpu.VMEM((total, tokens), bf16),
            pltpu.VMEM((tokens, total), bf16),
            pltpu.VMEM((3, total, COLS), bf16),
            pltpu.VMEM((total, ff), f32),
            pltpu.VMEM((total, ff), bf16),
            pltpu.VMEM((total, COLS), bf16),
            pltpu.VMEM((chunks, tokens, COLS), f32),
            pltpu.VMEM((chunks, tok, COLS), f32),
            pltpu.VMEM((chunks, tok, COLS), f32),
            pltpu.VMEM((chunks, tok, COLS), f32),
            pltpu.VMEM((chunks, tok, COLS), f32),
            pltpu.VMEM((tok, DIRECT), f32),
            pltpu.VMEM((tok, DIRECT), f32),
            pltpu.VMEM((tok, fs), bf16),
            pltpu.VMEM((tok, d_model), f32),
        ]
        sems = [pltpu.SemaphoreType.REGULAR, dma((2,)), dma((chunks,)), dma((chunks,)), dma((chunks,)), dma((5,)), dma((6,)), dma((6,))]
        sems += [dma((chunks,))] * 12 + [dma((2,))] * 2

        def kernel(*refs):
            pl.run_scoped(functools.partial(layer_kernel, (tok, top_k, local_e, slot, tokens), *refs), *sems)

        any_spec = pl.BlockSpec(memory_space=pltpu.HBM)
        return pl.pallas_call(
            kernel,
            out_shape=pltpu.VMEM((tok, d_model), bf16),
            in_specs=[any_spec] * 7,
            out_specs=pl.BlockSpec(memory_space=pltpu.VMEM),
            scratch_shapes=scratch,
            compiler_params=pltpu.CompilerParams(
                collective_id=0, has_side_effects=True, vmem_limit_bytes=VMEM_LIMIT),
        )(x_loc, idx_loc.T, gate_loc.T, w_in, w_out,
          shared_in.reshape(chunks, COLS, fs), shared_out.reshape(fs // COLS, COLS, d_model))

    tok_spec = P(('dp', 'ep'), None)
    expert_spec = P('ep', None, None)
    whole_spec = P(None, None)
    return jax.shard_map(
        local_layer, mesh=mesh,
        in_specs=(tok_spec, tok_spec, tok_spec, expert_spec, expert_spec, whole_spec, whole_spec),
        out_specs=tok_spec, check_vma=False)
```

```python
import functools
import math

import jax
import jax.numpy as jnp
from jax import lax
from jax.experimental import pallas as pl
from jax.experimental.pallas import tpu as pltpu
from jax.sharding import PartitionSpec as P

MESH = pl.DeviceIdType.MESH
LOAD_MULT = 3
SPOTS = (0, 2, 4, 6, 8, 10, 12, 13)
DIRECT = 128
EARLY = 12
LAG = 4
VMEM_LIMIT = 62500000
scope = jax.named_scope
COLS = 256
GELU_A = math.sqrt(2.0 / math.pi)
GELU_B = GELU_A * 0.044715


def gelu(z):
    return 0.5 * z * (1.0 + jnp.tanh(z * (GELU_A + GELU_B * (z * z))))


def dot(a, b):
    return jnp.dot(a, b, preferred_element_type=jnp.float32)


def layer_kernel(
    dims,
    x_hbm, idx_hbm, gate_hbm, win_hbm, wout_hbm, sin_hbm, sout_hbm,
    y_ref,
    x_all, win, wout, idx_all, gate_all, disp, comb, rows_in, acc, hidden, rows_out,
    part, sib_part, sib_fwd, link_out, link_in, direct_a, direct_b, shared_h, shared_u,
    *sems):
    (fence_sem, small_sem, x_sem, win_sem, wout_sem, shared_sem,
     meta_send, meta_recv, xl_send, xl_recv, xs_send, xs_recv, xf_send, xf_recv,
     ps_send, ps_recv, pf_send, pf_recv, pl_send, pl_recv, direct_send, direct_recv) = sems
    tok, top_k, local_e, slot, tokens = dims
    d_model, ff = win_hbm.shape[1], win_hbm.shape[2]
    chunks = d_model // COLS
    me = lax.axis_index('ep')
    chip, core = lax.div(me, 2), lax.rem(me, 2)
    sib = chip * 2 + (1 - core)
    partner = (1 - chip) * 2 + (1 - core)
    other = (1 - chip) * 2 + core
    peers = (sib, partner, other)

    def rows_of(dev):
        return pl.ds(pl.multiple_of(dev * tok, tok), tok)

    def remote(src, dst, send, recv, dev):
        return pltpu.make_async_remote_copy(
            src_ref=src, dst_ref=dst, send_sem=send, recv_sem=recv,
            device_id={'ep': dev}, device_id_type=MESH)

    def fence():
        pl.semaphore_signal(fence_sem, 1)
        pl.semaphore_wait(fence_sem, 1)

    idx_cp = pltpu.make_async_copy(idx_hbm, idx_all.at[me], small_sem.at[0])
    gate_cp = pltpu.make_async_copy(gate_hbm, gate_all.at[me], small_sem.at[1])
    x_cps = [pltpu.make_async_copy(x_hbm.at[:, pl.ds(k * COLS, COLS)], x_all.at[k, rows_of(me)], x_sem.at[k]) for k in range(chunks)]
    win_cps = [pltpu.make_async_copy(win_hbm.at[:, pl.ds(k * COLS, COLS), :], win.at[k], win_sem.at[k]) for k in range(chunks)]
    wout_cps = [pltpu.make_async_copy(wout_hbm.at[:, :, pl.ds(n * COLS, COLS)], wout.at[n], wout_sem.at[n]) for n in range(chunks)]
    barrier = pltpu.get_barrier_semaphore()
    for peer in peers:
        pl.semaphore_signal(barrier, inc=1, device_id={'ep': peer}, device_id_type=MESH)
    for cp in [idx_cp, gate_cp] + x_cps:
        cp.start()
    for cp in win_cps + wout_cps:
        fence()
        cp.start()

    with scope('w_small'):
        for cp in [idx_cp, gate_cp] + x_cps:
            cp.wait()
    with scope('w_barrier'):
        pl.semaphore_wait(barrier, 3)
    meta_cps = []
    for r, peer in enumerate(peers):
        meta_cps.append(remote(idx_all.at[me], idx_all.at[me], meta_send.at[r], meta_recv.at[r], peer))
        meta_cps.append(remote(gate_all.at[me], gate_all.at[me], meta_send.at[3 + r], meta_recv.at[3 + r], peer))
    for cp in meta_cps:
        cp.start()
    xl_cps, xs_cps, xf_cps = [], [], []
    for k in range(chunks):
        mine, theirs = x_all.at[k, rows_of(me)], x_all.at[k, rows_of(partner)]
        xl_cps.append(remote(mine, mine, xl_send.at[k], xl_recv.at[k], partner))
        xs_cps.append(remote(mine, mine, xs_send.at[k], xs_recv.at[k], sib))
        xf_cps.append(remote(theirs, theirs, xf_send.at[k], xf_recv.at[k], sib))
    for k in range(chunks):
        xl_cps[k].start()
        xs_cps[k].start()

    with scope('w_meta'):
        for cp in meta_cps:
            cp.wait_recv()
    group = tokens // tok
    idx_t = jnp.concatenate([idx_all[s] for s in range(group)], axis=1)
    gate_t = jnp.concatenate([gate_all[s] for s in range(group)], axis=1).astype(jnp.bfloat16).astype(jnp.float32)
    expert_id = lax.broadcasted_iota(jnp.int32, (local_e, tokens), 0) + me * local_e
    picked = jnp.zeros((local_e, tokens), jnp.float32)
    gates = jnp.zeros((local_e, tokens), jnp.float32)
    for j in range(top_k):
        hit = idx_t[j:j + 1, :] == expert_id
        picked = picked + jnp.where(hit, 1.0, 0.0)
        gates = gates + jnp.where(hit, gate_t[j:j + 1, :], 0.0)
    before = (lax.broadcasted_iota(jnp.int32, (tokens, tokens), 0) < lax.broadcasted_iota(jnp.int32, (tokens, tokens), 1))
    rank = dot(picked.astype(jnp.bfloat16), jnp.where(before, 1.0, 0.0).astype(jnp.bfloat16))
    rank = jnp.where(picked > 0.5, rank, -1.0)
    slot_id = lax.broadcasted_iota(jnp.int32, (slot, tokens), 0).astype(jnp.float32)
    for e in range(local_e):
        here = slot_id == rank[e:e + 1, :]
        disp[pl.ds(e * slot, slot), :] = jnp.where(here, 1.0, 0.0).astype(jnp.bfloat16)
        rows_out[pl.ds(e * slot, slot), :] = jnp.where(here, gates[e:e + 1, :], 0.0).astype(jnp.bfloat16)
    for i in range(local_e * slot // 256):
        comb[:, pl.ds(i * 256, 256)] = rows_out[pl.ds(i * 256, 256), :].T

    def forward(k):
        with scope(f'w_xl{k}'):
            xl_cps[k].wait_recv()
        xf_cps[k].start()

    def await_rows(k):
        with scope(f'w_xs{k}'):
            xs_cps[k].wait_recv()
        with scope(f'w_xf{k}'):
            xf_cps[k].wait_recv()

    def gather(k, piece, pieces):
        m = local_e * slot // pieces
        r = pl.ds(piece * m, m)
        rows_in[k % 3, r, :] = dot(disp[r, :], x_all[k]).astype(jnp.bfloat16)

    forward(0)
    forward(1)
    await_rows(0)
    gather(0, 0, 2)
    gather(0, 1, 2)
    def first(k, e):
        r = pl.ds(e * slot, slot)
        term = dot(rows_in[k % 3, r, :], win[k, e])
        if k == 0:
            acc[r, :] = term
        elif k + 2 < chunks:
            acc[r, :] = acc[r, :] + term
        else:
            term = term + dot(rows_in[(k + 1) % 3, r, :], win[k + 1, e])
            hidden[r, :] = gelu(acc[r, :] + term).astype(jnp.bfloat16)

    def second(n, e, total):
        r = pl.ds(e * slot, slot)
        rows_out[r, :] = dot(hidden[r, :], wout[n, e]).astype(jnp.bfloat16)
        ready = e * slot // COLS if e + 1 < local_e else local_e * slot // COLS
        for i in range(max(e - 1, 0) * slot // COLS, ready):
            c = pl.ds(i * COLS, COLS)
            term = dot(comb[:, c], rows_out[c, :])
            total = term if total is None else total + term
        return total

    for k in range(chunks - 2):
        if k + 3 < chunks:
            forward(k + 2)
        await_rows(k + 1)
        if k + 4 == chunks:
            forward(chunks - 1)
        if k + 3 == chunks:
            await_rows(chunks - 1)
        with scope(f'w_win{k}'):
            win_cps[k].wait()
        for e in range(local_e):
            first(k, e)
            if e in SPOTS:
                gather(k + 1, SPOTS.index(e), len(SPOTS))
                if k + 3 == chunks:
                    gather(chunks - 1, SPOTS.index(e), len(SPOTS))
    for k in range(chunks - 2, chunks):
        with scope(f'w_win{k}'):
            win_cps[k].wait()
    with scope('w_wout0'):
        wout_cps[0].wait()
    total = None
    for e in range(local_e + LAG):
        if e < local_e:
            first(chunks - 2, e)
        if e >= LAG:
            total = second(0, e - LAG, total)

    shared_cps = []

    def load_shared():
        for j in range(2):
            shared_cps.append(pltpu.make_async_copy(sin_hbm.at[:, :, pl.ds(j * ff, ff)], win.at[:, j], shared_sem.at[j]))
        for j in range(3):
            shared_cps.append(pltpu.make_async_copy(
                sout_hbm.at[:, :, pl.ds(j * ff, ff)], win.at[pl.ds(0, sout_hbm.shape[0]), 2 + j], shared_sem.at[2 + j]))
        for cp in shared_cps:
            cp.start()

    head, rest = pl.ds(0, DIRECT), pl.ds(DIRECT, COLS - DIRECT)
    da_cp = remote(part.at[0, rows_of(partner), head], direct_a, direct_send.at[0], direct_recv.at[0], partner)
    db_cp = remote(part.at[0, rows_of(other), head], direct_b, direct_send.at[1], direct_recv.at[1], other)
    ps_cps = [remote(part.at[n, rows_of(sib)], sib_part.at[n], ps_send.at[n], ps_recv.at[n], sib) for n in range(chunks)]
    pf_cps = [remote(part.at[0, rows_of(other), rest], sib_fwd.at[0, :, rest], pf_send.at[0], pf_recv.at[0], sib)]
    pl_cps = [remote(link_out.at[0, :, rest], link_in.at[0, :, rest], pl_send.at[0], pl_recv.at[0], partner)]
    for n in range(1, chunks):
        pf_cps.append(remote(part.at[n, rows_of(other)], sib_fwd.at[n], pf_send.at[n], pf_recv.at[n], sib))
        pl_cps.append(remote(link_out.at[n], link_in.at[n], pl_send.at[n], pl_recv.at[n], partner))

    def send_back(n):
        with scope(f'w_pf{n}'):
            pf_cps[n].wait_recv()
        c = pl.ds(0, COLS) if n else rest
        link_out[n, :, c] = part[n, rows_of(partner), c] + sib_fwd[n, :, c]
        pl_cps[n].start()

    for n in range(chunks):
        if n:
            with scope(f'w_wout{n}'):
                wout_cps[n].wait()
        if n:
            total = None
            for e in range(local_e):
                if n == 2 and e == EARLY:
                    send_back(1)
                total = second(n, e, total)
        part[n] = total
        pf_cps[n].start()
        if n == 0:
            da_cp.start()
            db_cp.start()
        ps_cps[n].start()
        if n == 0:
            load_shared()
        if n and n != 2:
            send_back(n - 1)
    send_back(chunks - 1)

    with scope('w_shared'):
        for cp in shared_cps:
            cp.wait()
    for j in range(2):
        s = dot(x_all[0, rows_of(me), :], win[0, j])
        for k in range(1, chunks):
            s = s + dot(x_all[k, rows_of(me), :], win[k, j])
        shared_h[:, pl.ds(j * ff, ff)] = gelu(s).astype(jnp.bfloat16)
    for j in range(3):
        u = dot(shared_h[:, 0:COLS], win[0, 2 + j])
        for i in range(1, 4):
            u = u + dot(shared_h[:, pl.ds(i * COLS, COLS)], win[i, 2 + j])
        shared_u[:, pl.ds(j * ff, ff)] = u

    for n in range(chunks):
        with scope(f'w_ps{n}'):
            ps_cps[n].wait_recv()
        mine = shared_u[:, pl.ds(n * COLS, COLS)] + part[n, rows_of(me), :] + sib_part[n]
        with scope(f'w_pl{n}'):
            pl_cps[n].wait_recv()
        if n:
            y_ref[:, pl.ds(n * COLS, COLS)] = (mine + link_in[n]).astype(jnp.bfloat16)
        else:
            da_cp.wait_recv()
            db_cp.wait_recv()
            y_ref[:, head] = (mine[:, :DIRECT] + (direct_a[...] + direct_b[...])).astype(jnp.bfloat16)
            y_ref[:, rest] = (mine[:, DIRECT:] + link_in[0, :, rest]).astype(jnp.bfloat16)
    with scope('w_sends'):
        for cp in [da_cp, db_cp] + meta_cps + xl_cps + xs_cps + xf_cps + ps_cps + pf_cps + pl_cps:
            cp.wait_send()


def solution(mesh):
    group = mesh.shape['ep']

    def local_layer(x_loc, idx_loc, gate_loc, w_in, w_out, shared_in, shared_out):
        tok, top_k = idx_loc.shape
        local_e, d_model, ff = w_in.shape
        fs = shared_in.shape[1]
        tokens = tok * group
        cap = min(tok, LOAD_MULT * tok * top_k // (local_e * group))
        slot = -(-cap * group // 16) * 16
        total = local_e * slot
        chunks = d_model // COLS
        bf16, f32 = jnp.bfloat16, jnp.float32
        dma = pltpu.SemaphoreType.DMA
        scratch = [
            pltpu.VMEM((chunks, tokens, COLS), bf16),
            pltpu.VMEM((chunks, local_e, COLS, ff), bf16),
            pltpu.VMEM((chunks, local_e, ff, COLS), bf16),
            pltpu.VMEM((group, top_k, tok), jnp.int32),
            pltpu.VMEM((group, top_k, tok), f32),
            pltpu.VMEM((total, tokens), bf16),
            pltpu.VMEM((tokens, total), bf16),
            pltpu.VMEM((3, total, COLS), bf16),
            pltpu.VMEM((total, ff), f32),
            pltpu.VMEM((total, ff), bf16),
            pltpu.VMEM((total, COLS), bf16),
            pltpu.VMEM((chunks, tokens, COLS), f32),
            pltpu.VMEM((chunks, tok, COLS), f32),
            pltpu.VMEM((chunks, tok, COLS), f32),
            pltpu.VMEM((chunks, tok, COLS), f32),
            pltpu.VMEM((chunks, tok, COLS), f32),
            pltpu.VMEM((tok, DIRECT), f32),
            pltpu.VMEM((tok, DIRECT), f32),
            pltpu.VMEM((tok, fs), bf16),
            pltpu.VMEM((tok, d_model), f32),
        ]
        sems = [pltpu.SemaphoreType.REGULAR, dma((2,)), dma((chunks,)), dma((chunks,)), dma((chunks,)), dma((5,)), dma((6,)), dma((6,))]
        sems += [dma((chunks,))] * 12 + [dma((2,))] * 2

        def kernel(*refs):
            pl.run_scoped(functools.partial(layer_kernel, (tok, top_k, local_e, slot, tokens), *refs), *sems)

        any_spec = pl.BlockSpec(memory_space=pltpu.HBM)
        return pl.pallas_call(
            kernel,
            out_shape=pltpu.VMEM((tok, d_model), bf16),
            in_specs=[any_spec] * 7,
            out_specs=pl.BlockSpec(memory_space=pltpu.VMEM),
            scratch_shapes=scratch,
            compiler_params=pltpu.CompilerParams(
                collective_id=0, has_side_effects=True, vmem_limit_bytes=VMEM_LIMIT),
        )(x_loc, idx_loc.T, gate_loc.T, w_in, w_out,
          shared_in.reshape(chunks, COLS, fs), shared_out.reshape(fs // COLS, COLS, d_model))

    tok_spec = P(('dp', 'ep'), None)
    expert_spec = P('ep', None, None)
    whole_spec = P(None, None)
    return jax.shard_map(
        local_layer, mesh=mesh,
        in_specs=(tok_spec, tok_spec, tok_spec, expert_spec, expert_spec, whole_spec, whole_spec),
        out_specs=tok_spec, check_vma=False)
```
